128 devices in a mesh: row: 16 (over y, z), col: 8 (over x, core).
Axes of the slice: x: 4, y: 4, z: 4, core: 2. Of those that a mesh axis runs over, the one named last changes fastest.
Arguments:
- node_latent: bfloat16 [32768, 512], P(('row', 'col')), may hold values from -6 to 6
- edge_latent: bfloat16 [262144, 512], P(('row', 'col')), may hold values from -6 to 6
- node_cotangent: bfloat16 [32768, 512], P(('row', 'col')), may hold values from -6 to 6
- edge_cotangent: bfloat16 [262144, 512], P(('row', 'col')), may hold values from -6 to 6
- w_edge_in: bfloat16 [1536, 512], replicated, may hold values from -0.15625 to 0.15625
- w_edge_out: bfloat16 [512, 512], replicated, may hold values from -0.25 to 0.25
- w_node_in: bfloat16 [1024, 512], replicated, may hold values from -0.1875 to 0.1875
- w_node_out: bfloat16 [512, 512], replicated, may hold values from -0.25 to 0.25
- sender_code: int32 [262144], P(('row', 'col')), may hold values from 0 to 1535, as said below
- receiver: int32 [262144], P(('row', 'col')), may hold values from 0 to 255
- near_list: int32 [128, 4, 64], P(('row', 'col')), may hold values from 0 to 255
- far_list: int32 [128, 128, 8], P(('row', 'col')), may hold values from 0 to 255
Outputs:
- node_new: bfloat16 [32768, 512], P(('row', 'col'))
- edge_new: bfloat16 [262144, 512], P(('row', 'col'))
- grad_node: bfloat16 [32768, 512], P(('row', 'col'))
- grad_edge: bfloat16 [262144, 512], P(('row', 'col'))
- grad_edge_in: float32 [1536, 512], P(('row', 'col'))
- grad_edge_out: float32 [512, 512], P(('row', 'col'))
- grad_node_in: float32 [1024, 512], P(('row', 'col'))
- grad_node_out: float32 [512, 512], P(('row', 'col'))
The draws below stay inside these ranges and needn't reach their ends.
Inputs may be any that keep to these rules, and one draw needn't show every extreme that they name: `sender_code`: for each block d and each device p, the far codes of block d that name p use the first c of the 8 slots, 1 <= c <= 8, c drawn for each pair, and every block uses all 8 slots of some device. Every local code, every near code and every used far code is read by at least one edge of its block.
All inputs are finite; a program needn't handle non-finite values.
Results may differ from the reference program's by a relative error of at most 0.015.
Values may be sent and summed in bfloat16 or wider, within the bound.
No kernel may reach another device: no remote copies, remote signals or barrier semaphores. Data moves between devices by JAX's collectives and lax.ppermute only.
A program may use at most 128 MiB of HBM per device.

```python
import math
import jax
import jax.numpy as jnp
from jax import lax

D = 512
NODE_DEV = 256
NEAR = 64
FAR = 8
PEERS = 128
EDGE_DEV = 2048
NODES = 32768
EDGES = 262144
N_ROW = 16
N_COL = 8


def draw_sender_code(key, part):
    codes = NODE_DEV + 4 * NEAR + PEERS * FAR
    counts = jax.random.randint(jax.random.fold_in(key, 101), (PEERS, PEERS), 1, FAR + 1).astype(jnp.int32)
    offsets = jax.random.randint(jax.random.fold_in(key, 102), (PEERS,), 0, PEERS).astype(jnp.int32)
    devices = jnp.arange(PEERS, dtype=jnp.int32)
    full_peer = (devices + offsets) % PEERS
    counts = jnp.where(devices[None, :] == full_peer[:, None], FAR, counts)
    keys = jax.random.split(jax.random.fold_in(key, 103), PEERS)

    def one_block(count_row, block_key):
        base = jnp.arange(codes, dtype=jnp.int32)
        far_pos = base - (NODE_DEV + 4 * NEAR)
        peer = jnp.clip(far_pos // FAR, 0, PEERS - 1)
        slot = far_pos % FAR
        used = (far_pos < 0) | (slot < count_row[peer])
        spare = jax.random.randint(jax.random.fold_in(block_key, 1), (codes,), 0, NODE_DEV).astype(jnp.int32)
        mapped = jnp.where(used, base, spare)
        picks = jax.random.randint(jax.random.fold_in(block_key, 2), (EDGE_DEV - codes,), 0, codes)
        joined = jnp.concatenate([mapped, mapped[picks]])
        order = jax.random.permutation(jax.random.fold_in(block_key, 3), EDGE_DEV)
        return joined[order].astype(jnp.int32)
    return jax.vmap(one_block)(counts, keys).reshape(-1)


def place_ends(drawn, rng, low, largest):
    dims = drawn.shape
    spot = [jax.random.randint(jax.random.fold_in(rng, axis), (), 0, dims[axis]) for axis in range(len(dims))]
    drawn = drawn.at[tuple(spot)].set(low)
    longest = dims.index(max(dims))
    spot[longest] = (spot[longest] + 1) % dims[longest]
    return drawn.at[tuple(spot)].set(largest)


def block_scale(key, shape, cuts, low, top_value):
    def one(axis_at, blocks):
        draws = jax.random.uniform(jax.random.fold_in(jax.random.fold_in(key, 6), axis_at), (blocks,), jnp.float32, low / len(cuts), top_value / len(cuts))
        return jnp.repeat(jnp.exp(draws), shape[axis_at] // blocks).reshape((-1,) + (1,) * (len(shape) - axis_at - 1))

    level = one(*cuts[0])
    for cut in cuts[1:]:
        level = level * one(*cut)
    return level


def noise(own_key, dims, scale, bound, shards=(), kind=jnp.bfloat16):
    values = scale * jax.random.normal(own_key, dims, jnp.float32)
    if shards:
        values = values * block_scale(own_key, dims, shards, -0.22, 0.18)
    return jnp.clip(values, -bound, bound).astype(kind)


def setup_inputs(seed: int = 0) -> dict:
    streams_of = jax.random.split(jax.random.key(seed), 13)
    return {
        "node_latent": noise(streams_of[0], (NODES, D), 1.0, 6.0, ((0, 128),)),
        "edge_latent": noise(streams_of[1], (EDGES, D), 1.0, 6.0, ((0, 128),)),
        "node_cotangent": noise(streams_of[2], (NODES, D), 1.0, 6.0, ((0, 128),)),
        "edge_cotangent": noise(streams_of[3], (EDGES, D), 1.0, 6.0, ((0, 128),)),
        "w_edge_in": noise(streams_of[4], (3 * D, D), (3 * D) ** -0.5, 0.15625),
        "w_edge_out": noise(streams_of[5], (D, D), D ** -0.5, 0.25),
        "w_node_in": noise(streams_of[6], (2 * D, D), (2 * D) ** -0.5, 0.1875),
        "w_node_out": noise(streams_of[7], (D, D), D ** -0.5, 0.25),
        "sender_code": draw_sender_code(jax.random.fold_in(streams_of[12], 71), 0),
        "receiver": place_ends(jax.random.randint(streams_of[9], (EDGES,), 0, NODE_DEV), jax.random.fold_in(streams_of[9], 1), 0, NODE_DEV - 1).astype(jnp.int32),
        "near_list": place_ends(jax.random.randint(streams_of[10], (PEERS, 4, NEAR), 0, NODE_DEV), jax.random.fold_in(streams_of[10], 1), 0, NODE_DEV - 1).astype(jnp.int32),
        "far_list": place_ends(jax.random.randint(streams_of[11], (PEERS, PEERS, FAR), 0, NODE_DEV), jax.random.fold_in(streams_of[11], 1), 0, NODE_DEV - 1).astype(jnp.int32),
    }


EPS = 1e-05

def layer_norm(value):
    mean = lax.optimization_barrier(jnp.mean(value, -1, keepdims=True))
    centred = value - mean
    recip = lax.rsqrt(lax.optimization_barrier(jnp.mean(centred * centred, -1, keepdims=True)) + EPS)
    return centred * recip

def norm_grad(value, grad):
    mean = lax.optimization_barrier(jnp.mean(value, -1, keepdims=True))
    centred = value - mean
    recip = lax.rsqrt(lax.optimization_barrier(jnp.mean(centred * centred, -1, keepdims=True)) + EPS)
    normed = centred * recip
    inner = grad - lax.optimization_barrier(jnp.mean(grad, -1, keepdims=True)) - normed * lax.optimization_barrier(jnp.mean(grad * normed, -1, keepdims=True))
    return recip * inner

def silu_grad(value):
    sigma = jax.nn.sigmoid(value)
    return sigma * (1.0 + value * (1.0 - sigma))

def plain_dot(left, right):
    return jnp.dot(left, right, preferred_element_type=jnp.float32)

def back_dot(left, weight):
    return lax.dot_general(left, weight, (((1,), (1,)), ((), ())), preferred_element_type=jnp.float32)

def cross_dot(left, right):
    return lax.dot_general(left, right, (((0,), (0,)), ((), ())), preferred_element_type=jnp.float32)

def sender_index(sender_code, near_list, far_list):
    codes = sender_code.reshape(PEERS, EDGE_DEV).astype(jnp.int32)
    device = jnp.arange(PEERS, dtype=jnp.int32)[:, None]
    grid_row = device // N_COL
    grid_col = device % N_COL
    near_pos = codes - NODE_DEV
    kind = jnp.clip(near_pos // NEAR, 0, 3).astype(jnp.int32)
    near_slot = (near_pos % NEAR).astype(jnp.int32)
    src_row = jnp.where(kind == 0, (grid_row - 1) % N_ROW, jnp.where(kind == 1, (grid_row + 1) % N_ROW, grid_row))
    src_col = jnp.where(kind == 2, (grid_col - 1) % N_COL, jnp.where(kind == 3, (grid_col + 1) % N_COL, grid_col))
    near_src = (src_row * N_COL + src_col).astype(jnp.int32)
    near_node = near_list[near_src, kind, near_slot]
    far_pos = codes - NODE_DEV - 4 * NEAR
    peer = jnp.clip(far_pos // FAR, 0, PEERS - 1).astype(jnp.int32)
    far_slot = (far_pos % FAR).astype(jnp.int32)
    far_node = far_list[peer, jnp.broadcast_to(device, codes.shape), far_slot]
    local = device * NODE_DEV + codes
    near_global = near_src * NODE_DEV + near_node
    far_global = peer * NODE_DEV + far_node
    chosen = jnp.where(codes < NODE_DEV, local, jnp.where(far_pos < 0, near_global, far_global))
    return chosen.astype(jnp.int32)

def reference(node_latent, edge_latent, node_cotangent, edge_cotangent, w_edge_in, w_edge_out, w_node_in, w_node_out, sender_code, receiver, near_list, far_list):
    width = D
    senders = sender_index(sender_code, near_list, far_list)
    local_recv = receiver.reshape(PEERS, EDGE_DEV).astype(jnp.int32)
    global_recv = (local_recv + jnp.arange(PEERS, dtype=jnp.int32)[:, None] * NODE_DEV).astype(jnp.int32)
    edge_blocks = edge_latent.reshape(PEERS, EDGE_DEV, width)
    cot_blocks = edge_cotangent.reshape(PEERS, EDGE_DEV, width)
    w_e = w_edge_in[:width]
    w_s = w_edge_in[width:2 * width]
    w_r = w_edge_in[2 * width:]
    node_ids = jnp.arange(NODE_DEV, dtype=jnp.int32)[:, None]

    def edge_front(edges, send_idx, recv_idx):
        sent_rows = jnp.take(node_latent, send_idx, axis=0)
        recv_rows = jnp.take(node_latent, recv_idx, axis=0)
        edge_pre = plain_dot(edges, w_e) + plain_dot(sent_rows, w_s) + plain_dot(recv_rows, w_r)
        edge_hidden = jax.nn.silu(edge_pre).astype(jnp.bfloat16)
        edge_mid = plain_dot(edge_hidden, w_edge_out)
        return (sent_rows, recv_rows, edge_pre, edge_hidden, edge_mid)

    def forward_block(block):
        edges, send_idx, recv_idx, recv_local = block
        parts = edge_front(edges, send_idx, recv_idx)
        edge_new = (edges.astype(jnp.float32) + layer_norm(parts[4])).astype(jnp.bfloat16)
        onehot = (recv_local[None, :] == node_ids).astype(jnp.bfloat16)
        gathered = plain_dot(onehot, edge_new).astype(jnp.bfloat16)
        return (edge_new, gathered)
    edge_new, gathered = lax.map(forward_block, (edge_blocks, senders, global_recv, local_recv))
    edge_new = edge_new.reshape(EDGES, width)
    gathered = gathered.reshape(NODES, width)
    node_pre = plain_dot(node_latent, w_node_in[:width]) + plain_dot(gathered, w_node_in[width:])
    node_hidden = jax.nn.silu(node_pre).astype(jnp.bfloat16)
    node_mid = plain_dot(node_hidden, w_node_out)
    node_new = (node_latent.astype(jnp.float32) + layer_norm(node_mid)).astype(jnp.bfloat16)
    node_delta = norm_grad(node_mid, node_cotangent.astype(jnp.float32)).astype(jnp.bfloat16)
    node_pre_delta = (back_dot(node_delta, w_node_out) * silu_grad(node_pre)).astype(jnp.bfloat16)
    gathered_grad = back_dot(node_pre_delta, w_node_in[width:])
    node_in_grad = back_dot(node_pre_delta, w_node_in[:width])
    grad_node_in = jnp.concatenate([cross_dot(node_latent, node_pre_delta), cross_dot(gathered, node_pre_delta)], 0)
    grad_node_out = cross_dot(node_hidden, node_delta)

    def backward_block(carry, block):
        node_acc, acc_in, acc_out = carry
        edges, cots, send_idx, recv_idx = block
        sent_rows, recv_rows, edge_pre, edge_hidden, edge_mid = edge_front(edges, send_idx, recv_idx)
        edge_total = cots.astype(jnp.float32) + jnp.take(gathered_grad, recv_idx, axis=0)
        edge_delta = norm_grad(edge_mid, edge_total).astype(jnp.bfloat16)
        edge_pre_delta = (back_dot(edge_delta, w_edge_out) * silu_grad(edge_pre)).astype(jnp.bfloat16)
        grad_edge = (edge_total + back_dot(edge_pre_delta, w_e)).astype(jnp.bfloat16)
        node_acc = node_acc.at[send_idx].add(back_dot(edge_pre_delta, w_s))
        node_acc = node_acc.at[recv_idx].add(back_dot(edge_pre_delta, w_r))
        block_in = jnp.concatenate([cross_dot(edges, edge_pre_delta), cross_dot(sent_rows, edge_pre_delta), cross_dot(recv_rows, edge_pre_delta)], 0)
        acc_in = acc_in + block_in
        acc_out = acc_out + cross_dot(edge_hidden, edge_delta)
        return ((node_acc, acc_in, acc_out), grad_edge)
    start = (jnp.zeros((NODES, width), jnp.float32), jnp.zeros((3 * width, width), jnp.float32), jnp.zeros((width, width), jnp.float32))
    (node_acc, acc_in, acc_out), grad_edge = lax.scan(backward_block, start, (edge_blocks, cot_blocks, senders, global_recv))
    grad_edge = grad_edge.reshape(EDGES, width)
    grad_node = (node_cotangent.astype(jnp.float32) + node_in_grad + node_acc).astype(jnp.bfloat16)
    edge_scale = 1.0 / math.sqrt(EDGES)
    node_scale = 1.0 / math.sqrt(NODES)
    return (node_new, edge_new, grad_node, grad_edge, acc_in * edge_scale, acc_out * edge_scale, grad_node_in * node_scale, grad_node_out * node_scale)
```

```python
import functools
import math

import jax
import jax.numpy as jnp
from jax import lax
from jax.experimental import pallas as pl
from jax.experimental.pallas import tpu as pltpu
from jax.sharding import PartitionSpec as P


EPS = 1e-05
BF = jnp.bfloat16
F32 = jnp.float32
AXES = ("row", "col")
D = 512
VMEM_LIMIT = 60 * 1024 * 1024


def dot(left, right):
    return jnp.dot(left, right, preferred_element_type=F32)


def dot_nt(left, right):
    return lax.dot_general(left, right, (((1,), (1,)), ((), ())), preferred_element_type=F32)


def dot_tn(left, right):
    return lax.dot_general(left, right, (((0,), (0,)), ((), ())), preferred_element_type=F32)


def iota(shape, dim):
    return lax.broadcasted_iota(jnp.int32, shape, dim)


def hot(mask):
    return jnp.where(mask, 1.0, 0.0).astype(BF)


def normed(value):
    mean = jnp.mean(value, -1, keepdims=True)
    centred = value - mean
    recip = lax.rsqrt(jnp.mean(centred * centred, -1, keepdims=True) + EPS)
    return centred * recip, recip


def norm_grad(y, recip, grad):
    inner = grad - jnp.mean(grad, -1, keepdims=True) - y * jnp.mean(grad * y, -1, keepdims=True)
    return recip * inner


def full(shape):
    return pl.BlockSpec(shape, lambda *_: (0,) * len(shape))


def params():
    return pltpu.CompilerParams(
        dimension_semantics=("arbitrary",), vmem_limit_bytes=VMEM_LIMIT
    )


def cost(flops, nbytes):
    return pl.CostEstimate(flops=int(flops), bytes_accessed=int(nbytes), transcendentals=0)


def column_of(table, groups, width):
    rows = groups * width
    pick = hot(iota((rows, groups), 0) // width == iota((rows, groups), 1))
    spread = dot(pick, table.astype(F32).astype(BF))
    keep = iota((rows, width), 0) % width == iota((rows, width), 1)
    return jnp.sum(jnp.where(keep, spread, 0.0), -1, keepdims=True).astype(jnp.int32)


def offer_kernel(node_ref, near_ref, far_ref, near_out, far_out):
    node = node_ref[...]
    rows = node.shape[0]
    near = near_ref[0]
    far = far_ref[0]
    near_col = column_of(near, *near.shape)
    far_col = column_of(far, *far.shape)
    n_near, n_far = near_col.shape[0], far_col.shape[0]
    far_out[...] = dot(hot(far_col == iota((n_far, rows), 1)), node).astype(BF)
    near_out[...] = dot(hot(near_col == iota((n_near, rows), 1)), node).astype(BF)


def local_kernel(
    rows, edge_ref, node_ref, we_ref, ws_ref, wr_ref, code_c, code_r, recv_c, recv_r,
    p_out, oh_out, oht_out, ohr_out, ohrt_out, nwr, nws,
):
    @pl.when(pl.program_id(0) == 0)
    def _():
        node = node_ref[...]
        nwr[...] = dot(node, wr_ref[...]).astype(BF)
        nws[...] = dot(node, ws_ref[...]).astype(BF)

    tile = edge_ref.shape[0]
    code = code_c[...]
    ohr = hot(recv_c[...] == iota((tile, rows), 1))
    ohl = hot(code == iota((tile, rows), 1))
    p_out[...] = dot(edge_ref[...], we_ref[...]) + dot(ohr, nwr[...]) + dot(ohl, nws[...])
    ohr_out[...] = ohr
    oh_out[...] = hot(code - rows == iota(oh_out.shape, 1))
    oht_out[...] = hot(code_r[...] == iota(oht_out.shape, 0))
    ohrt_out[...] = hot(recv_r[...] == iota(ohrt_out.shape, 0))


def main_kernel(
    steps, p_ref, oh_ref, edge_ref, ohrt_ref, cot_ref, ohr_ref, ohtf_ref,
    n0, n1, n2, n3, far_ref, ws_ref, wo_ref,
    node_ref, ncot_ref, va_ref, vb_ref, vo_ref,
    enew_out, nnew_out, epd_out, hid_out, ed_out, gg_out, fgrad_out, cs_out,
    ntot_out, gat_out, npd_out, nhid_out, nd_out,
    tws, acc, y_s, sp_s, rec_s, cs,
):
    step = pl.program_id(0)
    tile = edge_ref.shape[0]

    @pl.when(step == 0)
    def _():
        ws = ws_ref[...]
        width = n0.shape[0]
        for k, ref in enumerate((n0, n1, n2, n3)):
            tws[k * width : (k + 1) * width, :] = dot(ref[...], ws).astype(BF)
        tws[4 * width :, :] = dot(far_ref[...], ws).astype(BF)
        acc[...] = jnp.zeros_like(acc)

    @pl.when(step < steps)
    def _():
        pre = p_ref[...] + dot(oh_ref[...], tws[...])
        sigma = jax.nn.sigmoid(pre)
        hidden = pre * sigma
        sp = sigma + hidden * (1.0 - sigma)
        hid = hidden.astype(BF)
        mid = dot(hid, wo_ref[...])
        y, rec = normed(mid)
        enew = (edge_ref[...].astype(F32) + y).astype(BF)
        enew_out[...] = enew
        acc[...] += dot(ohrt_ref[...], enew)
        hid_out[pl.ds(step * tile, tile), :] = hid
        y_s[pl.ds(step * tile, tile), :] = y.astype(BF)
        sp_s[pl.ds(step * tile, tile), :] = sp.astype(BF)
        rec_s[pl.ds(step * tile, tile), :] = rec

    @pl.when(step == steps)
    def _():
        node = node_ref[...]
        gat = acc[...].astype(BF)
        pre = dot(node, va_ref[...]) + dot(gat, vb_ref[...])
        sigma = jax.nn.sigmoid(pre)
        hidden = pre * sigma
        hid = hidden.astype(BF)
        mid = dot(hid, vo_ref[...])
        y, rec = normed(mid)
        nnew_out[...] = (node.astype(F32) + y).astype(BF)
        ncot = ncot_ref[...].astype(F32)
        nd = norm_grad(y, rec, ncot).astype(BF)
        npd = (dot_nt(nd, vo_ref[...]) * (sigma + hidden * (1.0 - sigma))).astype(BF)
        gg_out[...] = dot_nt(npd, vb_ref[...]).astype(BF)
        ntot_out[...] = ncot + dot_nt(npd, va_ref[...])
        gat_out[...] = gat
        npd_out[...] = npd
        nhid_out[...] = hid
        nd_out[...] = nd
        cs[...] = jnp.zeros_like(cs)

    @pl.when(step >= steps)
    def _():
        at = (step - steps) * tile
        total = cot_ref[...].astype(F32) + dot(ohr_ref[...], gg_out[...])
        y = y_s[pl.ds(at, tile), :].astype(F32)
        ed = norm_grad(y, rec_s[pl.ds(at, tile), :], total).astype(BF)
        ed_out[...] = ed
        sp = sp_s[pl.ds(at, tile), :].astype(F32)
        epd = (dot_nt(ed, wo_ref[...]) * sp).astype(BF)
        epd_out[...] = epd
        cs[...] += dot(ohtf_ref[...], epd)

    @pl.when(step == 2 * steps - 1)
    def _():
        sums = cs[...].astype(BF)
        cs_out[...] = sums
        fgrad_out[...] = dot_nt(sums, ws_ref[...]).astype(BF)


def rest_kernel(
    steps, core_ref, edge_ref, cot_ref, ohr_ref, ohrt_ref, ohtl_ref, epd_ref, hid_ref, ed_ref,
    gg_ref, we_ref, ws_ref, wr_ref, node_ref, n0, n1, n2, n3, far_ref, cs_ref,
    ntot_ref, gat_ref, npd_ref, nhid_ref, nd_ref,
    ge_out, ntot_out, b0, b1, b2, b3, keep_out, give_out,
    dwe, dwo, csl, rs, g_in, g_out, v_in, v_out,
):
    step = pl.program_id(0)

    @pl.when(step == 0)
    def _():
        for ref in (dwe, dwo, csl, rs):
            ref[...] = jnp.zeros_like(ref)

    epd = epd_ref[...]
    total = cot_ref[...].astype(F32) + dot(ohr_ref[...], gg_ref[...])
    ge_out[...] = (total + dot_nt(epd, we_ref[...])).astype(BF)
    csl[...] += dot(ohtl_ref[...], epd)
    rs[...] += dot(ohrt_ref[...], epd)
    dwe[...] += dot_tn(edge_ref[...], epd)
    dwo[...] += dot_tn(hid_ref[...], ed_ref[...])

    @pl.when(step == steps - 1)
    def _():
        node = node_ref[...]
        rows = node.shape[0]
        width = n0.shape[0]
        loc = csl[:rows, :].astype(BF)
        near = csl[rows:, :].astype(BF)
        recv = rs[...].astype(BF)
        ws = ws_ref[...]
        ntot_out[...] = ntot_ref[...] + dot_nt(loc, ws) + dot_nt(recv, wr_ref[...])
        dws = dot_tn(node, loc) + dot_tn(far_ref[...], cs_ref[...])
        for k, (ref, back) in enumerate(zip((n0, n1, n2, n3), (b0, b1, b2, b3))):
            part = near[k * width : (k + 1) * width, :]
            back[...] = dot_nt(part, ws).astype(BF)
            dws = dws + dot_tn(ref[...], part)
        g_in[:D, :] = dwe[...].astype(BF)
        g_in[D : 2 * D, :] = dws.astype(BF)
        g_in[2 * D :, :] = dot_tn(node, recv).astype(BF)
        g_out[...] = dwo[...].astype(BF)
        npd = npd_ref[...]
        v_in[:D, :] = dot_tn(node, npd).astype(BF)
        v_in[D:, :] = dot_tn(gat_ref[...], npd).astype(BF)
        v_out[...] = dot_tn(nhid_ref[...], nd_ref[...]).astype(BF)

        me = core_ref[0]
        r = iota((256, 512), 0)
        q = iota((256, 512), 1)
        k = r // 32
        s = r % 32

        def picks(core):
            src = jnp.where(
                s < 12,
                24 * k + 12 * core + s,
                jnp.where(
                    s < 16,
                    192 + 8 * k + 4 * core + s - 12,
                    jnp.where(
                        s < 24,
                        256 + 16 * k + 8 * core + s - 16,
                        jnp.where(s < 28, 384 + 8 * k + 4 * core + s - 24, -1),
                    ),
                ),
            )
            return hot(src == q)

        mine = picks(me)
        other = picks(1 - me)
        for b in range(8):
            block = jnp.concatenate(
                [
                    g_in[192 * b : 192 * (b + 1), :],
                    g_out[64 * b : 64 * (b + 1), :],
                    v_in[128 * b : 128 * (b + 1), :],
                    v_out[64 * b : 64 * (b + 1), :],
                    jnp.zeros((64, D), BF),
                ],
                0,
            )
            keep_out[256 * b : 256 * (b + 1), :] = dot(mine, block).astype(BF)
            give_out[256 * b : 256 * (b + 1), :] = dot(other, block).astype(BF)


def owner_kernel(ntot_ref, near_ref, far_ref, b0, b1, b2, b3, back_ref, out):
    rows = ntot_ref.shape[0]
    total = ntot_ref[...]
    total = total + dot(hot(far_ref[...] == iota((rows, far_ref.shape[1]), 0)), back_ref[...])
    near = jnp.concatenate([b0[...], b1[...], b2[...], b3[...]], 0)
    total = total + dot(hot(near_ref[...] == iota((rows, near_ref.shape[1]), 0)), near)
    out[...] = total.astype(BF)


def sum_kernel(edge_scale, node_scale, got_ref, o0, o1, o2, o3):
    total = jnp.sum(got_ref[...].astype(F32), 0)
    o0[...] = total[0:12] * edge_scale
    o1[...] = total[12:16] * edge_scale
    o2[...] = total[16:24] * node_scale
    o3[...] = total[24:28] * node_scale


def shards(
    node_latent, edge_latent, node_cotangent, edge_cotangent,
    w_edge_in, w_edge_out, w_node_in, w_node_out,
    sender_code, receiver, near_list, far_list,
):
    rows, width = node_latent.shape
    edges = edge_latent.shape[0]
    n_row, n_col = lax.axis_size("row"), lax.axis_size("col")
    peers = n_row * n_col
    near_w = near_list.shape[2]
    far_w = far_list.shape[2]
    n_near, n_far = 4 * near_w, peers * far_w
    codes = rows + n_near + n_far
    tile = 512
    steps = edges // tile
    sds = jax.ShapeDtypeStruct

    near_send, far_send = pl.pallas_call(
        offer_kernel,
        out_shape=(sds((n_near, width), BF), sds((n_far, width), BF)),
        name="offer",
    )(node_latent, near_list, far_list)

    far = lax.all_to_all(far_send.reshape(peers, far_w, width), AXES, 0, 0, tiled=True)
    far = far.reshape(n_far, width)
    moves = (("row", 1), ("row", -1), ("col", 1), ("col", -1))

    def shifted(value, axis, by):
        n = lax.axis_size(axis)
        return lax.ppermute(value, axis, [(i, (i + by) % n) for i in range(n)])

    near = [
        shifted(near_send[k * near_w : (k + 1) * near_w], axis, by)
        for k, (axis, by) in enumerate(moves)
    ]

    code_c = sender_code.reshape(edges, 1)
    code_r = sender_code.reshape(1, edges)
    recv_c = receiver.reshape(edges, 1)
    recv_r = receiver.reshape(1, edges)

    def rowed(cols):
        return pl.BlockSpec((tile, cols), lambda s: (s, 0))

    def laned(lead):
        return pl.BlockSpec((lead, tile), lambda s: (0, s))

    def wpart(k):
        return pl.BlockSpec((width, width), lambda *_: (k, 0))

    pre_local, oh, oht, ohr, ohrt = pl.pallas_call(
        functools.partial(local_kernel, rows),
        grid=(steps,),
        in_specs=[
            rowed(width), full((rows, width)), wpart(0), wpart(1), wpart(2),
            rowed(1), laned(1), rowed(1), laned(1),
        ],
        out_specs=[rowed(width), rowed(codes - rows), laned(codes), rowed(rows), laned(rows)],
        out_shape=(
            sds((edges, width), F32),
            sds((edges, codes - rows), BF),
            sds((codes, edges), BF),
            sds((edges, rows), BF),
            sds((rows, edges), BF),
        ),
        scratch_shapes=[pltpu.VMEM((rows, width), BF), pltpu.VMEM((rows, width), BF)],
        compiler_params=params(),
        cost_estimate=cost(2 * edges * width * (width + 2 * rows), 22e6),
        name="local",
    )(edge_latent, node_latent, w_edge_in, w_edge_in, w_edge_in, code_c, code_r, recv_c, recv_r)

    def first(cols):
        return pl.BlockSpec((tile, cols), lambda s: (jnp.minimum(s, steps - 1), 0))

    def second(cols):
        return pl.BlockSpec((tile, cols), lambda s: (jnp.maximum(s - steps, 0), 0))

    near_spec = [full((near_w, width))] * 4
    node_spec = full((rows, width))
    sq = full((width, width))
    (
        edge_new, node_new, epd, hid, ed, gg, far_grad, cs_far, ntot, gat, npd, nhid, nd,
    ) = pl.pallas_call(
        functools.partial(main_kernel, steps),
        grid=(2 * steps,),
        in_specs=[
            first(width), first(codes - rows), first(width),
            pl.BlockSpec((rows, tile), lambda s: (0, jnp.minimum(s, steps - 1))),
            second(width), second(rows),
            pl.BlockSpec((pl.Element(n_far), pl.Element(tile)), lambda s: (rows + n_near, jnp.maximum(s - steps, 0) * tile)),
            *near_spec, full((n_far, width)), wpart(1), sq,
            node_spec, node_spec, wpart(0), wpart(1), sq,
        ],
        out_specs=[
            first(width), node_spec, second(width), full((edges, width)), second(width),
            node_spec, full((n_far, width)), full((n_far, width)), node_spec,
            node_spec, node_spec, node_spec, node_spec,
        ],
        out_shape=(
            sds((edges, width), BF), sds((rows, width), BF),
            sds((edges, width), BF), sds((edges, width), BF), sds((edges, width), BF),
            sds((rows, width), BF), sds((n_far, width), BF), sds((n_far, width), BF),
            sds((rows, width), F32),
            sds((rows, width), BF), sds((rows, width), BF),
            sds((rows, width), BF), sds((rows, width), BF),
        ),
        scratch_shapes=[
            pltpu.VMEM((codes - rows, width), BF),
            pltpu.VMEM((rows, width), F32),
            pltpu.VMEM((edges, width), BF),
            pltpu.VMEM((edges, width), BF),
            pltpu.VMEM((edges, 1), F32),
            pltpu.VMEM((n_far, width), F32),
        ],
        compiler_params=params(),
        cost_estimate=cost(14e9, 30e6),
        name="middle",
    )(
        pre_local, oh, edge_latent, ohrt, edge_cotangent, ohr, oht,
        *near, far, w_edge_in, w_edge_out,
        node_latent, node_cotangent, w_node_in, w_node_in, w_node_out,
    )

    far_back = lax.all_to_all(far_grad.reshape(peers, far_w, width), AXES, 0, 0, tiled=True)
    far_back = far_back.reshape(n_far, width)

    core = (lax.axis_index("col") % 2).astype(jnp.int32).reshape(1)
    out_rows = 32 * (peers // 2)
    rest = pl.pallas_call(
        functools.partial(rest_kernel, steps),
        grid=(steps,),
        in_specs=[
            pl.BlockSpec(memory_space=pltpu.SMEM),
            rowed(width), rowed(width), rowed(rows), laned(rows),
            pl.BlockSpec((rows + n_near, tile), lambda s: (0, s)),
            rowed(width), rowed(width), rowed(width),
            node_spec, wpart(0), wpart(1), wpart(2), node_spec, *near_spec,
            full((n_far, width)), full((n_far, width)),
            node_spec, node_spec, node_spec, node_spec, node_spec,
        ],
        out_specs=[
            rowed(width), node_spec, *near_spec,
            full((out_rows, width)), full((out_rows, width)),
        ],
        out_shape=(
            sds((edges, width), BF), sds((rows, width), F32),
            *[sds((near_w, width), BF)] * 4,
            sds((out_rows, width), BF), sds((out_rows, width), BF),
        ),
        scratch_shapes=[
            pltpu.VMEM((width, width), F32), pltpu.VMEM((width, width), F32),
            pltpu.VMEM((rows + n_near, width), F32), pltpu.VMEM((rows, width), F32),
            pltpu.VMEM((3 * width, width), BF), pltpu.VMEM((width, width), BF),
            pltpu.VMEM((2 * width, width), BF), pltpu.VMEM((width, width), BF),
        ],
        compiler_params=params(),
        cost_estimate=cost(9e9, 24e6),
        name="rest",
    )
    grad_edge, ntot2, b0, b1, b2, b3, keep, give = rest(
        core, edge_latent, edge_cotangent, ohr, ohrt, oht, epd, hid, ed, gg,
        w_edge_in, w_edge_in, w_edge_in, node_latent, *near, far, cs_far,
        ntot, gat, npd, nhid, nd,
    )

    got = lax.ppermute(give, "col", [(i, i ^ 1) for i in range(n_col)])
    pair = (keep.astype(F32) + got.astype(F32)).astype(BF).reshape(peers // 2, 32, width)
    same_core = [[2 * i + c for i in range(peers // 2)] for c in range(2)]
    parts = lax.all_to_all(pair, AXES, 0, 0, axis_index_groups=same_core, tiled=True)

    back = [shifted(b, axis, -by) for b, (axis, by) in zip((b0, b1, b2, b3), moves)]
    grad_node = pl.pallas_call(
        owner_kernel,
        out_shape=sds((rows, width), BF),
        name="owner",
        cost_estimate=cost(4e8, 3e6),
    )(ntot2, near_list.reshape(1, n_near), far_list.reshape(1, n_far), *back, far_back)

    edge_scale = 1.0 / math.sqrt(edges * peers)
    node_scale = 1.0 / math.sqrt(rows * peers)
    g0, g1, g2, g3 = pl.pallas_call(
        functools.partial(sum_kernel, edge_scale, node_scale),
        out_shape=(
            sds((12, width), F32), sds((4, width), F32),
            sds((8, width), F32), sds((4, width), F32),
        ),
        name="total",
    )(parts)
    return (node_new, edge_new, grad_node, grad_edge, g0, g1, g2, g3)


def solution(mesh):
    both = P(AXES, None)
    in_specs = (
        both, both, both, both, P(), P(), P(), P(), P(AXES), P(AXES),
        P(AXES, None, None), P(AXES, None, None),
    )
    return jax.shard_map(
        shards, mesh=mesh, in_specs=in_specs, out_specs=(both,) * 8, check_vma=False
    )
```

```python
import functools
import math

import jax
import jax.numpy as jnp
from jax import lax
from jax.experimental import pallas as pl
from jax.experimental.pallas import tpu as pltpu
from jax.sharding import PartitionSpec as P


EPS = 1e-05
BF = jnp.bfloat16
F32 = jnp.float32
AXES = ("row", "col")
D = 512
EG = 1024
NG = 384
TILE = 512
SUB = 128
VMEM_LIMIT = 67043328


def dot(left, right):
    return jnp.dot(left, right, preferred_element_type=F32)


def dot_nt(left, right):
    return lax.dot_general(left, right, (((1,), (1,)), ((), ())), preferred_element_type=F32)


def dot_tn(left, right):
    return lax.dot_general(left, right, (((0,), (0,)), ((), ())), preferred_element_type=F32)


def iota(shape, dim):
    return lax.broadcasted_iota(jnp.int32, shape, dim)


def hot(mask):
    return jnp.where(mask, 1.0, 0.0).astype(BF)


def normed(value):
    mean = jnp.mean(value, -1, keepdims=True)
    centred = value - mean
    recip = lax.rsqrt(jnp.mean(centred * centred, -1, keepdims=True) + EPS)
    return centred * recip, recip


def norm_grad(y, recip, grad):
    inner = grad - jnp.mean(grad, -1, keepdims=True) - y * jnp.mean(grad * y, -1, keepdims=True)
    return recip * inner


def full(shape):
    return pl.BlockSpec(shape, lambda *_: (0,) * len(shape))


def params(axes=1):
    return pltpu.CompilerParams(
        dimension_semantics=("arbitrary",) * axes, vmem_limit_bytes=VMEM_LIMIT
    )


def cost(flops, nbytes):
    return pl.CostEstimate(flops=int(flops), bytes_accessed=int(nbytes), transcendentals=0)


def column_of(table_t, groups, width):
    rows = groups * width
    pick = hot(iota((rows, groups), 0) // width == iota((rows, groups), 1))
    spread = dot_nt(pick, table_t.astype(F32).astype(BF))
    keep = iota((rows, width), 0) % width == iota((rows, width), 1)
    return jnp.sum(jnp.where(keep, spread, 0.0), -1, keepdims=True).astype(jnp.int32)


def lanes_to_rows(blocks, count, first):
    pick = hot(iota((count, blocks.shape[0]), 0) // 128 + first == iota((count, blocks.shape[0]), 1))
    spread = dot(pick, blocks.astype(F32).astype(BF))
    keep = iota((count, 128), 0) % 128 == iota((count, 128), 1)
    return jnp.sum(jnp.where(keep, spread, 0.0), -1, keepdims=True).astype(jnp.int32)


def row_of(table_t, count, group_of):
    width, groups = table_t.shape
    pick = hot(iota((groups, count), 0) == group_of(iota((groups, count), 1) // width))
    spread = dot(table_t.astype(F32).astype(BF), pick)
    keep = iota((width, count), 1) % width == iota((width, count), 0)
    return jnp.sum(jnp.where(keep, spread, 0.0), 0, keepdims=True).astype(jnp.int32)


def offer_kernel(node_ref, near_ref, far_ref, n0, n1, n2, n3, far_out):
    node = node_ref[...]
    rows = node.shape[0]
    far_col = column_of(far_ref[...], far_ref.shape[1], far_ref.shape[0])
    far_out[...] = dot(hot(far_col == iota((far_col.shape[0], rows), 1)), node).astype(BF)
    near = near_ref[0]
    for k, out in enumerate((n0, n1, n2, n3)):
        pick = hot(near[k : k + 1, :] == iota((rows, near.shape[1]), 0))
        out[...] = dot_tn(pick, node).astype(BF)


def local_kernel(
    rows, edge_ref, node_ref, we_ref, ws_ref, wr_ref, code_b, code_r, recv_b, recv_r,
    p_out, oh_out, oht_out, ohr_out, ohrt_out, nwr, nws,
):
    @pl.when(pl.program_id(0) == 0)
    def _():
        node = node_ref[...]
        nwr[...] = dot(node, wr_ref[...]).astype(BF)
        nws[...] = dot(node, ws_ref[...]).astype(BF)

    tile = edge_ref.shape[0]
    first = pl.program_id(0) * (tile // 128)
    code = 256 * lanes_to_rows(code_b[...] // 256, tile, first)
    code = code + lanes_to_rows(code_b[...] % 256, tile, first)
    ohr = hot(lanes_to_rows(recv_b[...], tile, first) == iota((tile, rows), 1))
    ohl = hot(code == iota((tile, rows), 1))
    p_out[...] = dot(edge_ref[...], we_ref[...]) + dot(ohr, nwr[...]) + dot(ohl, nws[...])
    ohr_out[...] = ohr
    oh_out[...] = hot(code - rows == iota(oh_out.shape, 1))
    oht_out[...] = hot(code_r[...] == iota(oht_out.shape, 0))
    ohrt_out[...] = hot(recv_r[...] == iota(ohrt_out.shape, 0))


def forward_kernel(
    steps, sub, core_ref,
    p_ref, oh_ref, edge_ref, ohrt_ref,
    n0, n1, n2, n3, far_ref, ws_ref, wo_ref,
    node_ref, ncot_ref, va_ref, vb_ref, vo_ref,
    enew_out, y_out, sp_out, hid_out, rec_out,
    nnew_out, gg_out, ntot_out, keep_out, give_out,
    tws, acc, v_in, v_out,
):
    step = pl.program_id(0)
    tile = edge_ref.shape[0]
    width = n0.shape[0]

    @pl.when(step == 0)
    def _():
        ws = ws_ref[...]
        for k, ref in enumerate((n0, n1, n2, n3)):
            tws[k * width : (k + 1) * width, :] = dot(ref[...], ws).astype(BF)
        tws[4 * width :, :] = dot(far_ref[...], ws).astype(BF)
        acc[...] = jnp.zeros_like(acc)

    for lo in range(0, tile, sub):
        here = slice(lo, lo + sub)
        pre = p_ref[here, :] + dot(oh_ref[here, :], tws[...])
        sigma = jax.nn.sigmoid(pre)
        hidden = pre * sigma
        hid = hidden.astype(BF)
        hid_out[here, :] = hid
        sp_out[here, :] = (sigma + hidden * (1.0 - sigma)).astype(BF)
        mid = dot(hid, wo_ref[...])
        y, rec = normed(mid)
        y_out[here, :] = y.astype(BF)
        rec_out[here, :] = rec
        enew_out[here, :] = (edge_ref[here, :].astype(F32) + y).astype(BF)
    acc[...] += dot(ohrt_ref[...], enew_out[...])

    @pl.when(step == steps - 1)
    def _():
        node = node_ref[...]
        gat = acc[...].astype(BF)
        pre = dot(node, va_ref[...]) + dot(gat, vb_ref[...])
        sigma = jax.nn.sigmoid(pre)
        hidden = pre * sigma
        hid = hidden.astype(BF)
        mid = dot(hid, vo_ref[...])
        y, rec = normed(mid)
        nnew_out[...] = (node.astype(F32) + y).astype(BF)
        ncot = ncot_ref[...].astype(F32)
        nd = norm_grad(y, rec, ncot).astype(BF)
        npd = (dot_nt(nd, vo_ref[...]) * (sigma + hidden * (1.0 - sigma))).astype(BF)
        gg_out[...] = dot_nt(npd, vb_ref[...]).astype(BF)
        ntot_out[...] = ncot + dot_nt(npd, va_ref[...])
        v_in[:D, :] = dot_tn(node, npd).astype(BF)
        v_in[D:, :] = dot_tn(gat, npd).astype(BF)
        v_out[...] = dot_tn(hid, nd).astype(BF)
        pack_nodes(core_ref[0], v_in, v_out, keep_out, give_out)


def pack_nodes(me, v_in, v_out, keep_out, give_out):
    r = iota((128, 256), 0)
    q = iota((128, 256), 1)
    k, s = r // 8, r % 8
    whole = hot(8 * k + s == q)
    split = 128 + 4 * k + s % 4 == q
    low = hot(split & (s < 4))
    high = hot(split & (s >= 4))
    half, quarter = D // 2, D // 4
    for b in range(8):
        node = jnp.concatenate(
            [
                v_in[128 * b : 128 * (b + 1), :],
                v_out[64 * b : 64 * (b + 1), :],
                jnp.zeros((64, D), BF),
            ],
            0,
        )
        w = dot(whole, node)
        lo = dot(low, node)
        hi = dot(high, node)
        at = slice(128 * b, 128 * (b + 1))
        parts = [
            (
                w[:, half * h : half * (h + 1)],
                lo[:, half * h : half * h + quarter] + hi[:, half * h + quarter : half * (h + 1)],
            )
            for h in range(2)
        ]
        for out, first in ((keep_out, me), (give_out, 1 - me)):
            out[at, :half] = jnp.where(first == 0, parts[0][0], parts[1][0]).astype(BF)
            out[at, half:] = jnp.where(first == 0, parts[0][1], parts[1][1]).astype(BF)


def back_kernel(
    steps, sub, cot_ref, ohr_ref, y_ref, sp_ref, rec_ref, oht_ref, gg_ref, wo_ref, ws_ref,
    ed_out, epd_out, far_out, cs_out, cs,
):
    step = pl.program_id(0)
    tile = cot_ref.shape[0]

    @pl.when(step == 0)
    def _():
        cs[...] = jnp.zeros_like(cs)

    for lo in range(0, tile, sub):
        here = slice(lo, lo + sub)
        total = cot_ref[here, :].astype(F32) + dot(ohr_ref[here, :], gg_ref[...])
        ed = norm_grad(y_ref[here, :].astype(F32), rec_ref[here, :], total).astype(BF)
        ed_out[here, :] = ed
        epd_out[here, :] = (dot_nt(ed, wo_ref[...]) * sp_ref[here, :].astype(F32)).astype(BF)
    cs[...] += dot(oht_ref[...], epd_out[...])

    @pl.when(step == steps - 1)
    def _():
        sums = cs[...].astype(BF)
        cs_out[...] = sums
        far_out[:, :D] = dot_nt(sums, ws_ref[...]).astype(BF)


def add_kernel(big_ref, keep_ref, got_ref, out):
    out[...] = (keep_ref[...].astype(F32) + got_ref[...].astype(F32)).astype(BF)


def rest_kernel(
    steps, core_ref, edge_ref, epd_ref, hid_ref, ed_ref, ohtl_ref, ohrt_ref,
    node_ref, n0, n1, n2, n3, far_ref, cs_ref, ws_ref, wr_ref, ntot_ref,
    ntot_out, b0, b1, b2, b3, keep_out, give_out,
    csl, rs, dwe, dwo, g_in, g_out,
):
    step = pl.program_id(0)
    rows = node_ref.shape[0]
    width = n0.shape[0]

    @pl.when(step == 0)
    def _():
        for ref in (csl, rs, dwe, dwo):
            ref[...] = jnp.zeros_like(ref)

    epd = epd_ref[...]
    csl[...] += dot(ohtl_ref[...], epd)
    rs[...] += dot(ohrt_ref[...], epd)
    dwe[...] += dot_tn(edge_ref[...], epd)
    dwo[...] += dot_tn(hid_ref[...], ed_ref[...])

    @pl.when(step == steps - 1)
    def _():
        node = node_ref[...]
        ws = ws_ref[...]
        loc = csl[:rows, :].astype(BF)
        recv = rs[...].astype(BF)
        ntot_out[...] = ntot_ref[...] + dot_nt(loc, ws) + dot_nt(recv, wr_ref[...])
        dws = dot_tn(node, loc) + dot_tn(far_ref[...], cs_ref[...])
        for k, (ref, back) in enumerate(zip((n0, n1, n2, n3), (b0, b1, b2, b3))):
            part = csl[rows + k * width : rows + (k + 1) * width, :].astype(BF)
            back[...] = dot_nt(part, ws).astype(BF)
            dws = dws + dot_tn(ref[...], part)
        g_in[:D, :] = dwe[...].astype(BF)
        g_in[D : 2 * D, :] = dws.astype(BF)
        g_in[2 * D :, :] = dot_tn(node, recv).astype(BF)
        g_out[...] = dwo[...].astype(BF)
        pack_rows(core_ref[0], g_in, g_out, keep_out, give_out)


def pack_rows(me, g_in, g_out, keep_out, give_out):
    def place(r):
        group = r // 64
        return group, (r % 64) // 8, r % 8

    def select(count, depth, source, ok):
        r = iota((count, depth), 0)
        q = iota((count, depth), 1)
        group, k, s = place(r)
        return hot((source(group, k, s) == q) & ok(s))

    def core_of(half):
        return jnp.where(half == 0, me, 1 - me)

    def whole(s):
        return s >= 0

    def low(s):
        return s < 4

    def high(s):
        return s >= 4

    def edge_whole(g, k, s):
        return 24 * k + 12 * core_of(g) + s

    def edge_split(g, k, s):
        core = core_of(g // 2)
        return jnp.where(
            g % 2 == 0, 24 * k + 12 * core + 8 + s % 4, 192 + 8 * k + 4 * core + s % 4
        )

    e_all = select(128, 256, edge_whole, whole)
    e_low = select(256, 256, edge_split, low)
    e_high = select(256, 256, edge_split, high)
    half = D // 2
    for b in range(8):
        edge = jnp.concatenate(
            [g_in[192 * b : 192 * (b + 1), :], g_out[64 * b : 64 * (b + 1), :]], 0
        )
        ew = dot(e_all, edge).astype(BF)
        es = (dot(e_low, edge[:, :half]) + dot(e_high, edge[:, half:])).astype(BF)
        at = slice(64 * b, 64 * (b + 1))
        for i, out in enumerate((keep_out, give_out)):
            out[at, 0:D] = ew[64 * i : 64 * (i + 1), :]
            out[at, D : D + half] = es[128 * i : 128 * i + 64, :]
            out[at, D + half :] = es[128 * i + 64 : 128 * i + 128, :]


def edge_kernel(cot_ref, ohr_ref, epd_ref, gg_ref, we_ref, out):
    total = cot_ref[...].astype(F32) + dot(ohr_ref[...], gg_ref[...])
    out[...] = (total + dot_nt(epd_ref[...], we_ref[...])).astype(BF)


def pair_kernel(keep_ref, got_ref, out):
    out[...] = (keep_ref[...].astype(F32) + got_ref[...].astype(F32)).astype(BF)


def owner_kernel(node_scale, got_ref, ntot_ref, near_ref, far_ref, b0, b1, b2, b3, o2, o3, gn_out):
    rows = ntot_ref.shape[0]
    count = got_ref.shape[0]
    half, quarter = D // 2, D // 4
    sums = jnp.sum(got_ref[:, D:].astype(F32).reshape(count // 16, 16, NG), 0) * node_scale
    for h in range(2):
        part = sums[8 * h : 8 * (h + 1), :]
        o2[:, half * h : half * (h + 1)] = part[:, :half]
        o3[:, half * h : half * h + quarter] = part[0:4, half:]
        o3[:, half * h + quarter : half * (h + 1)] = part[4:8, half:]
    total = ntot_ref[...]
    near = near_ref[0]
    for k, ref in enumerate((b0, b1, b2, b3)):
        total = total + dot(hot(near[k : k + 1, :] == iota((rows, near.shape[1]), 0)), ref[...])
    owner = row_of(far_ref[...], count, lambda g: g)
    total = total + dot(hot(owner == iota((rows, count), 0)), got_ref[:, :D])
    gn_out[...] = total.astype(BF)


def edge_sum_kernel(edge_scale, got_ref, o0, o1):
    half = D // 2
    chips = got_ref.shape[0] // 8
    sums = jnp.sum(got_ref[...].astype(F32).reshape(chips, 8, EG), 0) * edge_scale
    o0[0:8, :] = sums[:, :D]
    o0[8:12, :half] = sums[0:4, D : D + half]
    o0[8:12, half:] = sums[4:8, D : D + half]
    o1[:, :half] = sums[0:4, D + half :]
    o1[:, half:] = sums[4:8, D + half :]


def shards(
    node_latent, edge_latent, node_cotangent, edge_cotangent,
    w_edge_in, w_edge_out, w_node_in, w_node_out,
    sender_code, receiver, near_list, far_list,
):
    rows, width = node_latent.shape
    edges = edge_latent.shape[0]
    n_row, n_col = lax.axis_size("row"), lax.axis_size("col")
    peers = n_row * n_col
    chips = peers // 2
    near_w = near_list.shape[2]
    far_w = far_list.shape[2]
    n_near, n_far = 4 * near_w, peers * far_w
    codes = rows + n_near + n_far
    tile = TILE
    steps = edges // tile
    sds = jax.ShapeDtypeStruct
    far_t = jnp.swapaxes(far_list[0], 0, 1)
    core = (lax.axis_index("col") % 2).astype(jnp.int32).reshape(1)
    smem = pl.BlockSpec(memory_space=pltpu.SMEM)

    *near_send, far_send = pl.pallas_call(
        offer_kernel,
        out_shape=(*[sds((near_w, width), BF)] * 4, sds((n_far, width), BF)),
        compiler_params=params(0),
        name="offer",
    )(node_latent, near_list, far_t)

    far = lax.all_to_all(far_send.reshape(peers, far_w, width), AXES, 0, 0, tiled=True)
    far = far.reshape(n_far, width)
    moves = (("row", 1), ("row", -1), ("col", 1), ("col", -1))

    def shifted(value, axis, by):
        n = lax.axis_size(axis)
        return lax.ppermute(value, axis, [(i, (i + by) % n) for i in range(n)])

    near = [shifted(part, axis, by) for part, (axis, by) in zip(near_send, moves)]

    def rowed(cols):
        return pl.BlockSpec((tile, cols), lambda s: (s, 0))

    def laned(lead):
        return pl.BlockSpec((lead, tile), lambda s: (0, s))

    def wpart(k):
        return pl.BlockSpec((width, width), lambda *_: (k, 0), pipeline_mode=pl.Buffered(1))

    def once(shape):
        return pl.BlockSpec(shape, lambda *_: (0,) * len(shape), pipeline_mode=pl.Buffered(1))

    blocks = full((edges // 128, 128))
    pre_local, oh, oht, ohr, ohrt = pl.pallas_call(
        functools.partial(local_kernel, rows),
        grid=(steps,),
        in_specs=[
            rowed(width), once((rows, width)), wpart(0), wpart(1), wpart(2),
            blocks, laned(1), blocks, laned(1),
        ],
        out_specs=[rowed(width), rowed(codes - rows), laned(codes), rowed(rows), laned(rows)],
        out_shape=(
            sds((edges, width), F32),
            sds((edges, codes - rows), BF),
            sds((codes, edges), BF),
            sds((edges, rows), BF),
            sds((rows, edges), BF),
        ),
        scratch_shapes=[pltpu.VMEM((rows, width), BF), pltpu.VMEM((rows, width), BF)],
        compiler_params=params(),
        cost_estimate=cost(2 * edges * width * (width + 2 * rows), 22e6),
        name="local",
    )(
        edge_latent, node_latent, w_edge_in, w_edge_in, w_edge_in,
        sender_code.reshape(edges // 128, 128), sender_code.reshape(1, edges),
        receiver.reshape(edges // 128, 128), receiver.reshape(1, edges),
    )

    near_spec = [once((near_w, width))] * 4
    node_spec = once((rows, width))
    sq = once((width, width))
    packed = once((8 * peers, NG))
    edge_bf = sds((edges, width), BF)
    edge_new, y, sp, hid, rec, node_new, gg, ntot, keep_n, give_n = pl.pallas_call(
        functools.partial(forward_kernel, steps, SUB),
        grid=(steps,),
        in_specs=[
            smem, rowed(width), rowed(codes - rows), rowed(width), laned(rows),
            *near_spec, once((n_far, width)), wpart(1), sq,
            node_spec, node_spec, wpart(0), wpart(1), sq,
        ],
        out_specs=[
            rowed(width), rowed(width), rowed(width), rowed(width), rowed(1),
            node_spec, node_spec, node_spec, packed, packed,
        ],
        out_shape=(
            edge_bf, edge_bf, edge_bf, edge_bf, sds((edges, 1), F32),
            sds((rows, width), BF), sds((rows, width), BF), sds((rows, width), F32),
            sds((8 * peers, NG), BF), sds((8 * peers, NG), BF),
        ),
        scratch_shapes=[
            pltpu.VMEM((codes - rows, width), BF),
            pltpu.VMEM((rows, width), F32),
            pltpu.VMEM((2 * width, width), BF),
            pltpu.VMEM((width, width), BF),
        ],
        compiler_params=params(),
        cost_estimate=cost(9e9, 24e6),
        name="forward",
    )(
        core, pre_local, oh, edge_latent, ohrt,
        *near, far, w_edge_in, w_edge_out,
        node_latent, node_cotangent, w_node_in, w_node_in, w_node_out,
    )

    def to_pair(value):
        return lax.ppermute(value, "col", [(i, i ^ 1) for i in range(n_col)])

    backward = pl.pallas_call(
        functools.partial(back_kernel, steps, SUB),
        grid=(steps,),
        in_specs=[
            rowed(width), rowed(rows), rowed(width), rowed(width), rowed(1),
            pl.BlockSpec(
                (pl.Element(n_far), pl.Element(tile)), lambda s: (rows + n_near, s * tile)
            ),
            node_spec, sq, wpart(1),
        ],
        out_specs=[
            rowed(width), rowed(width), once((n_far, width + NG)), once((n_far, width)),
        ],
        out_shape=(
            edge_bf, edge_bf, sds((n_far, width + NG), BF), sds((n_far, width), BF),
        ),
        scratch_shapes=[pltpu.VMEM((n_far, width), F32)],
        compiler_params=params(),
        cost_estimate=cost(6e9, 22e6),
        name="backward",
    )
    got_n = to_pair(give_n)
    ed, epd, far_grad, cs_far = backward(
        edge_cotangent, ohr, y, sp, rec, oht, gg, w_edge_out, w_edge_in
    )
    lanes = pl.BlockSpec((n_far, 128), lambda s: (0, s))
    beyond = pl.BlockSpec((n_far, 128), lambda s: (0, s + width // 128))
    sent = pl.pallas_call(
        add_kernel,
        grid=(NG // 128,),
        in_specs=[pl.BlockSpec(memory_space=pl.ANY), lanes, lanes],
        out_specs=beyond,
        out_shape=sds((n_far, width + NG), BF),
        input_output_aliases={0: 0},
        compiler_params=params(),
        name="add",
    )(far_grad, keep_n, got_n)
    rest = pl.pallas_call(
        functools.partial(rest_kernel, steps),
        grid=(steps,),
        in_specs=[
            smem, rowed(width), rowed(width), rowed(width), rowed(width),
            laned(rows + n_near), laned(rows),
            node_spec, *near_spec, once((n_far, width)), once((n_far, width)),
            wpart(1), wpart(2), node_spec,
        ],
        out_specs=[node_spec, *near_spec, once((8 * chips, EG)), once((8 * chips, EG))],
        out_shape=(
            sds((rows, width), F32), *[sds((near_w, width), BF)] * 4,
            sds((8 * chips, EG), BF), sds((8 * chips, EG), BF),
        ),
        scratch_shapes=[
            pltpu.VMEM((rows + n_near, width), F32),
            pltpu.VMEM((rows, width), F32),
            pltpu.VMEM((width, width), F32),
            pltpu.VMEM((width, width), F32),
            pltpu.VMEM((3 * width, width), BF),
            pltpu.VMEM((width, width), BF),
        ],
        compiler_params=params(),
        cost_estimate=cost(7e9, 14e6),
        name="rest",
    )
    returned = lax.all_to_all(sent.reshape(peers, far_w, width + NG), AXES, 0, 0, tiled=True)
    ntot, b0, b1, b2, b3, keep, give = rest(
        core, edge_latent, epd, hid, ed, oht, ohrt, node_latent, *near, far, cs_far,
        w_edge_in, w_edge_in, ntot,
    )

    edges_of = pl.pallas_call(
        edge_kernel,
        grid=(steps,),
        in_specs=[rowed(width), rowed(rows), rowed(width), node_spec, wpart(0)],
        out_specs=rowed(width),
        out_shape=sds((edges, width), BF),
        compiler_params=params(),
        cost_estimate=cost(6e9, 9e6),
        name="edges",
    )
    got = to_pair(give)
    back = [shifted(b, axis, -by) for b, (axis, by) in zip((b0, b1, b2, b3), moves)]
    grad_edge = edges_of(edge_cotangent, ohr, epd, gg, w_edge_in)

    part = pl.BlockSpec((2 * chips, EG), lambda s: (s, 0))
    pair = pl.pallas_call(
        pair_kernel,
        grid=(4,),
        in_specs=[part, part],
        out_specs=part,
        out_shape=sds((8 * chips, EG), BF),
        compiler_params=params(),
        name="pair",
    )(keep, got)
    same_core = [[2 * i + c for i in range(chips)] for c in range(2)]
    vm = pl.BlockSpec(memory_space=pltpu.VMEM)
    edge_scale = 1.0 / math.sqrt(edges * peers)
    node_scale = 1.0 / math.sqrt(rows * peers)
    parts = lax.all_to_all(
        pair.reshape(chips, 8, EG), AXES, 0, 0, axis_index_groups=same_core, tiled=True
    )
    g2, g3, grad_node = pl.pallas_call(
        functools.partial(owner_kernel, node_scale),
        in_specs=[vm] * 8,
        out_specs=[vm] * 3,
        out_shape=(
            sds((8, width), F32), sds((4, width), F32), sds((rows, width), BF),
        ),
        compiler_params=params(0),
        cost_estimate=cost(4e8, 5e6),
        name="owner",
    )(returned.reshape(n_far, width + NG), ntot, near_list, far_t, *back)
    g0, g1 = pl.pallas_call(
        functools.partial(edge_sum_kernel, edge_scale),
        in_specs=[vm],
        out_specs=[vm] * 2,
        out_shape=(sds((12, width), F32), sds((4, width), F32)),
        compiler_params=params(0),
        name="edgesum",
    )(parts.reshape(8 * chips, EG))
    return (node_new, edge_new, grad_node, grad_edge, g0, g1, g2, g3)


def solution(mesh):
    both = P(AXES, None)
    in_specs = (
        both, both, both, both, P(), P(), P(), P(), P(AXES), P(AXES),
        P(AXES, None, None), P(AXES, None, None),
    )
    return jax.shard_map(
        shards, mesh=mesh, in_specs=in_specs, out_specs=(both,) * 8, check_vma=False
    )
```

```python
import functools
import math

import jax
import jax.numpy as jnp
from jax import lax
from jax.experimental import pallas as pl
from jax.experimental.pallas import tpu as pltpu
from jax.sharding import PartitionSpec as P


EPS = 1e-05
BF = jnp.bfloat16
F32 = jnp.float32
AXES = ("row", "col")
D = 512
MIB = 1024 * 1024
GRADS = 1792
TILE = 512
SUB = 512
VMEM_LIMIT = 67043328


def dot(left, right):
    return jnp.dot(left, right, preferred_element_type=F32)


def dot_nt(left, right):
    return lax.dot_general(left, right, (((1,), (1,)), ((), ())), preferred_element_type=F32)


def dot_tn(left, right):
    return lax.dot_general(left, right, (((0,), (0,)), ((), ())), preferred_element_type=F32)


def iota(shape, dim):
    return lax.broadcasted_iota(jnp.int32, shape, dim)


def hot(mask):
    return jnp.where(mask, 1.0, 0.0).astype(BF)


def normed(value):
    mean = jnp.mean(value, -1, keepdims=True)
    centred = value - mean
    recip = lax.rsqrt(jnp.mean(centred * centred, -1, keepdims=True) + EPS)
    return centred * recip, recip


def norm_grad(y, recip, grad):
    inner = grad - jnp.mean(grad, -1, keepdims=True) - y * jnp.mean(grad * y, -1, keepdims=True)
    return recip * inner


def full(shape):
    return pl.BlockSpec(shape, lambda *_: (0,) * len(shape))


def params(mib=None, axes=1):
    return pltpu.CompilerParams(
        dimension_semantics=("arbitrary",) * axes, vmem_limit_bytes=mib * MIB if mib else VMEM_LIMIT
    )


def cost(flops, nbytes):
    return pl.CostEstimate(flops=int(flops), bytes_accessed=int(nbytes), transcendentals=0)


def column_of(table_t, groups, width):
    rows = groups * width
    pick = hot(iota((rows, groups), 0) // width == iota((rows, groups), 1))
    spread = dot_nt(pick, table_t.astype(F32).astype(BF))
    keep = iota((rows, width), 0) % width == iota((rows, width), 1)
    return jnp.sum(jnp.where(keep, spread, 0.0), -1, keepdims=True).astype(jnp.int32)


def lanes_to_rows(blocks, count, first):
    pick = hot(iota((count, blocks.shape[0]), 0) // 128 + first == iota((count, blocks.shape[0]), 1))
    spread = dot(pick, blocks.astype(F32).astype(BF))
    keep = iota((count, 128), 0) % 128 == iota((count, 128), 1)
    return jnp.sum(jnp.where(keep, spread, 0.0), -1, keepdims=True).astype(jnp.int32)


def row_of(table_t, count, group_of):
    width, groups = table_t.shape
    pick = hot(iota((groups, count), 0) == group_of(iota((groups, count), 1) // width))
    spread = dot(table_t.astype(F32).astype(BF), pick)
    keep = iota((width, count), 1) % width == iota((width, count), 0)
    return jnp.sum(jnp.where(keep, spread, 0.0), 0, keepdims=True).astype(jnp.int32)


def offer_kernel(node_ref, near_ref, far_ref, n0, n1, n2, n3, far_out):
    node = node_ref[...]
    rows = node.shape[0]
    far_col = column_of(far_ref[...], far_ref.shape[1], far_ref.shape[0])
    far_out[...] = dot(hot(far_col == iota((far_col.shape[0], rows), 1)), node).astype(BF)
    near = near_ref[0]
    for k, out in enumerate((n0, n1, n2, n3)):
        pick = hot(near[k : k + 1, :] == iota((rows, near.shape[1]), 0))
        out[...] = dot_tn(pick, node).astype(BF)


def local_kernel(
    rows, edge_ref, node_ref, we_ref, ws_ref, wr_ref, code_b, code_r, recv_b, recv_r,
    p_out, oh_out, oht_out, ohr_out, ohrt_out, nwr, nws,
):
    @pl.when(pl.program_id(0) == 0)
    def _():
        node = node_ref[...]
        nwr[...] = dot(node, wr_ref[...]).astype(BF)
        nws[...] = dot(node, ws_ref[...]).astype(BF)

    tile = edge_ref.shape[0]
    first = pl.program_id(0) * (tile // 128)
    code = 256 * lanes_to_rows(code_b[...] // 256, tile, first)
    code = code + lanes_to_rows(code_b[...] % 256, tile, first)
    ohr = hot(lanes_to_rows(recv_b[...], tile, first) == iota((tile, rows), 1))
    ohl = hot(code == iota((tile, rows), 1))
    p_out[...] = dot(edge_ref[...], we_ref[...]) + dot(ohr, nwr[...]) + dot(ohl, nws[...])
    ohr_out[...] = ohr
    oh_out[...] = hot(code - rows == iota(oh_out.shape, 1))
    oht_out[...] = hot(code_r[...] == iota(oht_out.shape, 0))
    ohrt_out[...] = hot(recv_r[...] == iota(ohrt_out.shape, 0))


def main_kernel(
    steps, sub, core_ref,
    p_ref, oh_ref, edge_ref, ohrt_ref, cot_ref, ohr_ref, oht_ref,
    n0, n1, n2, n3, far_ref, ws_ref, wr_ref, wo_ref,
    node_ref, ncot_ref, va_ref, vb_ref, vo_ref,
    enew_out, nnew_out, epd_out, gg_out, ntot_out, b0, b1, b2, b3, keep_out, give_out,
    tws, acc, y_s, sp_s, hid_s, rec_s, ed_s, cs, rs, dwe, dwo, v_in, v_out, g_in, g_out,
):
    step = pl.program_id(0)
    tile = edge_ref.shape[0]
    rows = node_ref.shape[0]
    width = n0.shape[0]
    base = rows + 4 * width

    @pl.when(step == 0)
    def _():
        ws = ws_ref[...]
        for k, ref in enumerate((n0, n1, n2, n3)):
            tws[k * width : (k + 1) * width, :] = dot(ref[...], ws).astype(BF)
        tws[4 * width :, :] = dot(far_ref[...], ws).astype(BF)
        acc[...] = jnp.zeros_like(acc)

    @pl.when(step < steps)
    def _():
        for lo in range(0, tile, sub):
            at = pl.ds(step * tile + lo, sub)
            here = slice(lo, lo + sub)
            pre = p_ref[here, :] + dot(oh_ref[here, :], tws[...])
            sigma = jax.nn.sigmoid(pre)
            hidden = pre * sigma
            hid = hidden.astype(BF)
            hid_s[at, :] = hid
            sp_s[at, :] = (sigma + hidden * (1.0 - sigma)).astype(BF)
            mid = dot(hid, wo_ref[...])
            y, rec = normed(mid)
            y_s[at, :] = y.astype(BF)
            rec_s[at, :] = rec
            enew_out[here, :] = (edge_ref[here, :].astype(F32) + y).astype(BF)
        acc[...] += dot(ohrt_ref[...], enew_out[...])

    @pl.when(step == steps)
    def _():
        node = node_ref[...]
        gat = acc[...].astype(BF)
        pre = dot(node, va_ref[...]) + dot(gat, vb_ref[...])
        sigma = jax.nn.sigmoid(pre)
        hidden = pre * sigma
        hid = hidden.astype(BF)
        mid = dot(hid, vo_ref[...])
        y, rec = normed(mid)
        nnew_out[...] = (node.astype(F32) + y).astype(BF)
        ncot = ncot_ref[...].astype(F32)
        nd = norm_grad(y, rec, ncot).astype(BF)
        npd = (dot_nt(nd, vo_ref[...]) * (sigma + hidden * (1.0 - sigma))).astype(BF)
        gg_out[...] = dot_nt(npd, vb_ref[...]).astype(BF)
        ntot_out[...] = ncot + dot_nt(npd, va_ref[...])
        v_in[:D, :] = dot_tn(node, npd).astype(BF)
        v_in[D:, :] = dot_tn(gat, npd).astype(BF)
        v_out[...] = dot_tn(hid, nd).astype(BF)
        for ref in (cs, rs, dwe, dwo):
            ref[...] = jnp.zeros_like(ref)

    @pl.when(step >= steps)
    def _():
        for lo in range(0, tile, sub):
            at = pl.ds((step - steps) * tile + lo, sub)
            here = slice(lo, lo + sub)
            total = cot_ref[here, :].astype(F32) + dot(ohr_ref[here, :], gg_out[...])
            y = y_s[at, :].astype(F32)
            ed = norm_grad(y, rec_s[at, :], total).astype(BF)
            ed_s[here, :] = ed
            epd_out[here, :] = (
                dot_nt(ed, wo_ref[...]) * sp_s[at, :].astype(F32)
            ).astype(BF)
        epd = epd_out[...]
        cs[...] += dot(oht_ref[...], epd)
        rs[...] += dot(ohrt_ref[...], epd)
        dwe[...] += dot_tn(edge_ref[...], epd)
        dwo[...] += dot_tn(hid_s[pl.ds((step - steps) * tile, tile), :], ed_s[...])

    @pl.when(step == 2 * steps - 1)
    def _():
        node = node_ref[...]
        ws = ws_ref[...]
        loc = cs[:rows, :].astype(BF)
        recv = rs[...].astype(BF)
        ntot_out[...] += dot_nt(loc, ws) + dot_nt(recv, wr_ref[...])
        dws = dot_tn(node, loc) + dot_tn(far_ref[...], cs[base:, :].astype(BF))
        for k, (ref, back) in enumerate(zip((n0, n1, n2, n3), (b0, b1, b2, b3))):
            part = cs[rows + k * width : rows + (k + 1) * width, :].astype(BF)
            back[...] = dot_nt(part, ws).astype(BF)
            dws = dws + dot_tn(ref[...], part)
        g_in[:D, :] = dwe[...].astype(BF)
        g_in[D : 2 * D, :] = dws.astype(BF)
        g_in[2 * D :, :] = dot_tn(node, recv).astype(BF)
        g_out[...] = dwo[...].astype(BF)

        me = core_ref[0]
        fgrad = dot_nt(cs[base:, :].astype(BF), ws)
        chips = keep_out.shape[0] // 8
        fgrad = fgrad.reshape(chips, 16, D)
        even = fgrad[:, :8, :].reshape(8 * chips, D)
        odd = fgrad[:, 8:, :].reshape(8 * chips, D)
        keep_out[:, GRADS:] = jnp.where(me == 0, even, odd).astype(BF)
        give_out[:, GRADS:] = jnp.where(me == 0, odd, even).astype(BF)
        pack_rows(me, g_in, g_out, v_in, v_out, keep_out, give_out)


def pack_rows(me, g_in, g_out, v_in, v_out, keep_out, give_out):
    def place(r):
        group = r // 64
        return group, (r % 64) // 8, r % 8

    def select(count, depth, source, ok):
        r = iota((count, depth), 0)
        q = iota((count, depth), 1)
        group, k, s = place(r)
        return hot((source(group, k, s) == q) & ok(s))

    def core_of(half):
        return jnp.where(half == 0, me, 1 - me)

    def whole(s):
        return s >= 0

    def low(s):
        return s < 4

    def high(s):
        return s >= 4

    def edge_whole(g, k, s):
        return 24 * k + 12 * core_of(g) + s

    def edge_split(g, k, s):
        core = core_of(g // 2)
        return jnp.where(
            g % 2 == 0, 24 * k + 12 * core + 8 + s % 4, 192 + 8 * k + 4 * core + s % 4
        )

    def node_whole(g, k, s):
        return 16 * k + 8 * core_of(g) + s

    def node_split(g, k, s):
        return 128 + 8 * k + 4 * core_of(g) + s % 4

    e_all = select(128, 256, edge_whole, whole)
    e_low = select(256, 256, edge_split, low)
    e_high = select(256, 256, edge_split, high)
    n_all = select(128, 256, node_whole, whole)
    n_low = select(128, 256, node_split, low)
    n_high = select(128, 256, node_split, high)
    half = D // 2
    for b in range(8):
        edge = jnp.concatenate(
            [g_in[192 * b : 192 * (b + 1), :], g_out[64 * b : 64 * (b + 1), :]], 0
        )
        node = jnp.concatenate(
            [
                v_in[128 * b : 128 * (b + 1), :],
                v_out[64 * b : 64 * (b + 1), :],
                jnp.zeros((64, D), BF),
            ],
            0,
        )
        ew = dot(e_all, edge).astype(BF)
        es = (dot(e_low, edge[:, :half]) + dot(e_high, edge[:, half:])).astype(BF)
        nw = dot(n_all, node).astype(BF)
        ns = (dot(n_low, node[:, :half]) + dot(n_high, node[:, half:])).astype(BF)
        at = slice(64 * b, 64 * (b + 1))
        for i, out in enumerate((keep_out, give_out)):
            out[at, 0:D] = ew[64 * i : 64 * (i + 1), :]
            out[at, D : 2 * D] = nw[64 * i : 64 * (i + 1), :]
            out[at, 2 * D : 2 * D + half] = es[128 * i : 128 * i + 64, :]
            out[at, 2 * D + half : 3 * D] = es[128 * i + 64 : 128 * i + 128, :]
            out[at, 3 * D : 3 * D + half] = ns[64 * i : 64 * (i + 1), :]


def edge_kernel(cot_ref, ohr_ref, epd_ref, gg_ref, we_ref, out):
    total = cot_ref[...].astype(F32) + dot(ohr_ref[...], gg_ref[...])
    out[...] = (total + dot_nt(epd_ref[...], we_ref[...])).astype(BF)


def pair_kernel(keep_ref, got_ref, out):
    mine = keep_ref[:, :GRADS].astype(F32)
    out[:, :GRADS] = (mine + got_ref[:, :GRADS].astype(F32)).astype(BF)
    out[:, GRADS : GRADS + D] = keep_ref[:, GRADS:]
    out[:, GRADS + D :] = got_ref[:, GRADS:]


def final_kernel(
    edge_scale, node_scale, core_ref, got_ref, ntot_ref, near_ref, far_ref, b0, b1, b2, b3,
    o0, o1, o2, o3, gn_out,
):
    me = core_ref[0]
    rows = ntot_ref.shape[0]
    half = D // 2
    chips = got_ref.shape[0] // 8

    def summed(lo, hi):
        return jnp.sum(got_ref[:, lo:hi].astype(F32).reshape(chips, 8, hi - lo), 0)

    whole = summed(0, D) * edge_scale
    split = summed(2 * D, 2 * D + half) * edge_scale
    o0[0:8, :] = whole
    o0[8:12, :half] = split[0:4]
    o0[8:12, half:] = split[4:8]
    split = summed(2 * D + half, 3 * D) * edge_scale
    o1[:, :half] = split[0:4]
    o1[:, half:] = split[4:8]
    o2[...] = summed(D, 2 * D) * node_scale
    split = summed(3 * D, 3 * D + half) * node_scale
    o3[:, :half] = split[0:4]
    o3[:, half:] = split[4:8]

    total = ntot_ref[...]
    near = near_ref[0]
    for k, ref in enumerate((b0, b1, b2, b3)):
        total = total + dot(hot(near[k : k + 1, :] == iota((rows, near.shape[1]), 0)), ref[...])
    far = far_ref[...]
    count = got_ref.shape[0]
    for i in range(2):
        core = me if i == 0 else 1 - me
        owner = row_of(far, count, lambda g: 2 * g + core)
        pick = hot(owner == iota((rows, count), 0))
        total = total + dot(pick, got_ref[:, GRADS + i * D : GRADS + (i + 1) * D])
    gn_out[...] = total.astype(BF)


def shards(
    node_latent, edge_latent, node_cotangent, edge_cotangent,
    w_edge_in, w_edge_out, w_node_in, w_node_out,
    sender_code, receiver, near_list, far_list,
):
    rows, width = node_latent.shape
    edges = edge_latent.shape[0]
    n_row, n_col = lax.axis_size("row"), lax.axis_size("col")
    peers = n_row * n_col
    chips = peers // 2
    near_w = near_list.shape[2]
    far_w = far_list.shape[2]
    n_near, n_far = 4 * near_w, peers * far_w
    codes = rows + n_near + n_far
    tile = TILE
    steps = edges // tile
    sds = jax.ShapeDtypeStruct
    far_t = jnp.swapaxes(far_list[0], 0, 1)
    core = (lax.axis_index("col") % 2).astype(jnp.int32).reshape(1)
    smem = pl.BlockSpec(memory_space=pltpu.SMEM)

    *near_send, far_send = pl.pallas_call(
        offer_kernel,
        out_shape=(*[sds((near_w, width), BF)] * 4, sds((n_far, width), BF)),
        compiler_params=pltpu.CompilerParams(vmem_limit_bytes=VMEM_LIMIT),
        name="offer",
    )(node_latent, near_list, far_t)

    far = lax.all_to_all(far_send.reshape(peers, far_w, width), AXES, 0, 0, tiled=True)
    far = far.reshape(n_far, width)
    moves = (("row", 1), ("row", -1), ("col", 1), ("col", -1))

    def shifted(value, axis, by):
        n = lax.axis_size(axis)
        return lax.ppermute(value, axis, [(i, (i + by) % n) for i in range(n)])

    near = [shifted(part, axis, by) for part, (axis, by) in zip(near_send, moves)]

    def rowed(cols):
        return pl.BlockSpec((tile, cols), lambda s: (s, 0))

    def laned(lead):
        return pl.BlockSpec((lead, tile), lambda s: (0, s))

    def wpart(k):
        return pl.BlockSpec((width, width), lambda *_: (k, 0), pipeline_mode=pl.Buffered(1))

    def once(shape):
        return pl.BlockSpec(shape, lambda *_: (0,) * len(shape), pipeline_mode=pl.Buffered(1))

    blocks = full((edges // 128, 128))
    pre_local, oh, oht, ohr, ohrt = pl.pallas_call(
        functools.partial(local_kernel, rows),
        grid=(steps,),
        in_specs=[
            rowed(width), once((rows, width)), wpart(0), wpart(1), wpart(2),
            blocks, laned(1), blocks, laned(1),
        ],
        out_specs=[rowed(width), rowed(codes - rows), laned(codes), rowed(rows), laned(rows)],
        out_shape=(
            sds((edges, width), F32),
            sds((edges, codes - rows), BF),
            sds((codes, edges), BF),
            sds((edges, rows), BF),
            sds((rows, edges), BF),
        ),
        scratch_shapes=[pltpu.VMEM((rows, width), BF), pltpu.VMEM((rows, width), BF)],
        compiler_params=params(),
        cost_estimate=cost(2 * edges * width * (width + 2 * rows), 22e6),
        name="local",
    )(
        edge_latent, node_latent, w_edge_in, w_edge_in, w_edge_in,
        sender_code.reshape(edges // 128, 128), sender_code.reshape(1, edges),
        receiver.reshape(edges // 128, 128), receiver.reshape(1, edges),
    )

    def first(cols):
        return pl.BlockSpec((tile, cols), lambda s: (jnp.minimum(s, steps - 1), 0))

    def second(cols):
        return pl.BlockSpec((tile, cols), lambda s: (jnp.maximum(s - steps, 0), 0))

    def either(s):
        return jnp.where(s < steps, s, s - steps)

    near_spec = [once((near_w, width))] * 4
    node_spec = once((rows, width))
    sq = once((width, width))
    packed = once((8 * chips, GRADS + width))
    edge_new, node_new, epd, gg, ntot, b0, b1, b2, b3, keep, give = pl.pallas_call(
        functools.partial(main_kernel, steps, SUB),
        grid=(2 * steps,),
        in_specs=[
            smem,
            first(width), first(codes - rows),
            pl.BlockSpec((tile, width), lambda s: (either(s), 0)),
            pl.BlockSpec((rows, tile), lambda s: (0, either(s))),
            second(width), second(rows),
            pl.BlockSpec((codes, tile), lambda s: (0, jnp.maximum(s - steps, 0))),
            *near_spec, once((n_far, width)), wpart(1), wpart(2), sq,
            node_spec, node_spec, wpart(0), wpart(1), sq,
        ],
        out_specs=[
            first(width), node_spec, second(width), node_spec, node_spec,
            *near_spec, packed, packed,
        ],
        out_shape=(
            sds((edges, width), BF), sds((rows, width), BF), sds((edges, width), BF),
            sds((rows, width), BF), sds((rows, width), F32),
            *[sds((near_w, width), BF)] * 4,
            *[sds((8 * chips, GRADS + width), BF)] * 2,
        ),
        scratch_shapes=[
            pltpu.VMEM((codes - rows, width), BF),
            pltpu.VMEM((rows, width), F32),
            pltpu.VMEM((edges, width), BF),
            pltpu.VMEM((edges, width), BF),
            pltpu.VMEM((edges, width), BF),
            pltpu.VMEM((edges, 1), F32),
            pltpu.VMEM((tile, width), BF),
            pltpu.VMEM((codes, width), F32),
            pltpu.VMEM((rows, width), F32),
            pltpu.VMEM((width, width), F32),
            pltpu.VMEM((width, width), F32),
            pltpu.VMEM((2 * width, width), BF),
            pltpu.VMEM((width, width), BF),
            pltpu.VMEM((3 * width, width), BF),
            pltpu.VMEM((width, width), BF),
        ],
        compiler_params=params(),
        cost_estimate=cost(20e9, 30e6),
        name="middle",
    )(
        core, pre_local, oh, edge_latent, ohrt, edge_cotangent, ohr, oht,
        *near, far, w_edge_in, w_edge_in, w_edge_out,
        node_latent, node_cotangent, w_node_in, w_node_in, w_node_out,
    )

    edges_of = pl.pallas_call(
        edge_kernel,
        grid=(steps,),
        in_specs=[rowed(width), rowed(rows), rowed(width), node_spec, wpart(0)],
        out_specs=rowed(width),
        out_shape=sds((edges, width), BF),
        compiler_params=params(16),
        cost_estimate=cost(6e9, 9e6),
        name="edges",
    )
    got = lax.ppermute(give, "col", [(i, i ^ 1) for i in range(n_col)])
    grad_edge = edges_of(edge_cotangent, ohr, epd, gg, w_edge_in)
    back = [shifted(b, axis, -by) for b, (axis, by) in zip((b0, b1, b2, b3), moves)]

    half = 4 * chips
    part = pl.BlockSpec((half, GRADS + width), lambda s: (s, 0))
    pair = pl.pallas_call(
        pair_kernel,
        grid=(2,),
        in_specs=[part, part],
        out_specs=pl.BlockSpec((half, GRADS + 2 * width), lambda s: (s, 0)),
        out_shape=sds((8 * chips, GRADS + 2 * width), BF),
        compiler_params=params(16),
        name="pair",
    )(keep, got)
    same_core = [[2 * i + c for i in range(chips)] for c in range(2)]
    parts = lax.all_to_all(
        pair.reshape(chips, 8, GRADS + 2 * width), AXES, 0, 0,
        axis_index_groups=same_core, tiled=True,
    )

    edge_scale = 1.0 / math.sqrt(edges * peers)
    node_scale = 1.0 / math.sqrt(rows * peers)
    vm = pl.BlockSpec(memory_space=pltpu.VMEM)
    g0, g1, g2, g3, grad_node = pl.pallas_call(
        functools.partial(final_kernel, edge_scale, node_scale),
        in_specs=[smem] + [vm] * 8,
        out_specs=[vm] * 5,
        out_shape=(
            sds((12, width), F32), sds((4, width), F32),
            sds((8, width), F32), sds((4, width), F32), sds((rows, width), BF),
        ),
        compiler_params=pltpu.CompilerParams(vmem_limit_bytes=VMEM_LIMIT),
        name="final",
    )(core, parts.reshape(8 * chips, GRADS + 2 * width), ntot, near_list, far_t, *back)
    return (node_new, edge_new, grad_node, grad_edge, g0, g1, g2, g3)


def solution(mesh):
    both = P(AXES, None)
    in_specs = (
        both, both, both, both, P(), P(), P(), P(), P(AXES), P(AXES),
        P(AXES, None, None), P(AXES, None, None),
    )
    return jax.shard_map(
        shards, mesh=mesh, in_specs=in_specs, out_specs=(both,) * 8, check_vma=False
    )
```
